32 devices in a mesh: gx: 4 (over y, x), gy: 4 (over z), gz: 2 (over core).
Axes of the slice: x: 2, y: 2, z: 4, core: 2. Of those that a mesh axis runs over, the one named last changes fastest.
Arguments:
- nodal_scalar_values: float32 [3, 32, 32, 4096], P(None, 'gx', 'gy', 'gz'), may hold values from -6 to 6
- geometry: float32 [6, 4, 4, 512], P(None, 'gx', 'gy', 'gz'), may hold values from -1.2 to 4, as said below
Outputs:
- assembled: float32 [3, 32, 32, 4096], P(None, 'gx', 'gy', 'gz')
The draws below stay inside these ranges and needn't reach their ends.
Inputs may be any that keep to these rules, and one draw needn't show every extreme that they name: `geometry`: G00, G11 and G22 are positive; each off-diagonal factor is at most 0.3 times the root of the product of its two diagonal factors in magnitude.
All inputs are finite; a program needn't handle non-finite values.
Results may differ from the reference program's by a relative error of at most 0.00007.
Values sent between devices are 32-bit elements; how exact they have to be, the bound alone decides.
A program may use at most 64 MiB of HBM per device.

```python
import math
import jax
import jax.numpy as jnp
import numpy as np
from jax import lax

COMPONENTS = 3
ELEMENTS_FIRST = 4
ELEMENTS_SECOND = 4
ELEMENTS_THIRD = 512


def draw_geometry(key, part):
    element_grid_shape = (ELEMENTS_FIRST, ELEMENTS_SECOND, ELEMENTS_THIRD)
    key_list = jax.random.split(key, 2)
    diagonal = jnp.exp(jax.random.uniform(key_list[0], (3,) + element_grid_shape, jnp.float32, math.log(0.5), math.log(2.0)))
    coupling = jax.random.uniform(key_list[1], (3,) + element_grid_shape, jnp.float32, -0.3, 0.3)
    cross_xy = coupling[0] * jnp.sqrt(diagonal[0] * diagonal[1])
    cross_xz = coupling[1] * jnp.sqrt(diagonal[0] * diagonal[2])
    cross_yz = coupling[2] * jnp.sqrt(diagonal[1] * diagonal[2])
    return jnp.stack([diagonal[0], diagonal[1], diagonal[2], cross_xy, cross_xz, cross_yz]).astype(jnp.float32)


def level_of(own_key, extent, cuts, low, high):
    factor_of, own = 1.0, jax.random.fold_in(own_key, 6)
    for axis_at, blocks in cuts:
        steps = jnp.exp(jax.random.uniform(jax.random.fold_in(own, axis_at), (blocks,), jnp.float32, low / len(cuts), high / len(cuts)))
        factor_of = factor_of * jnp.repeat(steps, extent[axis_at] // blocks).reshape([-1 if axis == axis_at else 1 for axis in range(len(extent))])
    return factor_of


def gaussian(key, shape, scale, most, pieces=(), held_as=jnp.bfloat16):
    level = level_of(key, shape, pieces, -0.22, 0.18) if pieces else 1.0
    entries = jax.random.normal(key, shape, jnp.float32) * scale * level
    return jnp.minimum(jnp.maximum(entries, -most), most).astype(held_as)


def setup_inputs(seed: int = 0) -> dict:
    key_of = jax.random.split(jax.random.key(seed), 3)
    return {
        "nodal_scalar_values": gaussian(key_of[0], (COMPONENTS, 8 * ELEMENTS_FIRST, 8 * ELEMENTS_SECOND, 8 * ELEMENTS_THIRD), 1.0, 6.0, ((1, 4), (2, 4), (3, 2)), jnp.float32),
        "geometry": draw_geometry(jax.random.fold_in(key_of[2], 71), 0),
    }


interior_points = [-0.8717401485096066, -0.5917001814331423, -0.2092992179024789, 0.2092992179024789, 0.5917001814331423, 0.8717401485096066]


def legendre_seven(point):
    previous = 1.0
    current = point
    for order in range(1, 7):
        following = ((2 * order + 1) * point * current - order * previous) / (order + 1)
        previous = current
        current = following
    return current


def gll_tables():
    degree = 7
    points = [-1.0] + interior_points + [1.0]
    values = [legendre_seven(point) for point in points]
    node_count = degree + 1
    weights = np.array([2.0 / (degree * (degree + 1) * value * value) for value in values])
    derivative = np.zeros((node_count, node_count))
    for row_index in range(node_count):
        for col_index in range(node_count):
            if row_index != col_index:
                derivative[row_index, col_index] = values[row_index] / (values[col_index] * (points[row_index] - points[col_index]))
    derivative[0, 0] = -degree * (degree + 1) / 4.0
    derivative[node_count - 1, node_count - 1] = degree * (degree + 1) / 4.0
    return derivative, weights


def apply_axis(field_in, matrix, direction):
    length = field_in.shape[direction]
    block_size = math.gcd(length, 128)
    big_table = jnp.kron(jnp.eye(block_size // 8, dtype=jnp.float32), matrix)
    dim_list = list(field_in.shape)
    folded_shape = dim_list[:direction] + [length // block_size, block_size] + dim_list[direction + 1:]
    folded_field = field_in.reshape(folded_shape)
    patterns = ["nbyz,ab->nayz", "xnbz,ab->xnaz", "xynb,ab->xyna"]
    result = jnp.einsum(patterns[direction], folded_field, big_table, precision=lax.Precision.HIGHEST)
    return result.reshape(field_in.shape)


def expand(field_component, target):
    elem_x, elem_y, elem_z = field_component.shape
    spread = jnp.broadcast_to(field_component[:, None, :, None, :, None], (elem_x, 8, elem_y, 8, elem_z, 8))
    return spread.reshape(target)


def stiffness(field_in, geometry):
    derivative, weights = gll_tables()
    matrix = jnp.asarray(derivative, jnp.float32)
    weight_row = jnp.asarray(weights, jnp.float32)
    size_x, size_y, size_z = field_in.shape
    weight_x = jnp.tile(weight_row, size_x // 8)
    weight_y = jnp.tile(weight_row, size_y // 8)
    weight_z = jnp.tile(weight_row, size_z // 8)
    node_weight = weight_x[:, None, None] * weight_y[None, :, None] * weight_z[None, None, :]
    grad_x = apply_axis(field_in, matrix, 0)
    grad_y = apply_axis(field_in, matrix, 1)
    grad_z = apply_axis(field_in, matrix, 2)
    factors = [expand(geometry[index], field_in.shape) for index in range(6)]
    flux_x = node_weight * (factors[0] * grad_x + factors[3] * grad_y + factors[4] * grad_z)
    flux_y = node_weight * (factors[3] * grad_x + factors[1] * grad_y + factors[5] * grad_z)
    flux_z = node_weight * (factors[4] * grad_x + factors[5] * grad_y + factors[2] * grad_z)
    transposed = matrix.T
    return apply_axis(flux_x, transposed, 0) + apply_axis(flux_y, transposed, 1) + apply_axis(flux_z, transposed, 2)


def combine(middle, below_plane, above_plane, direction):
    length = middle.shape[direction]
    from_above = jnp.concatenate([lax.slice_in_dim(middle, 1, length, axis=direction), above_plane], axis=direction)
    from_below = jnp.concatenate([below_plane, lax.slice_in_dim(middle, 0, length - 1, axis=direction)], axis=direction)
    position = lax.broadcasted_iota(jnp.int32, middle.shape, direction) % 8
    return middle + jnp.where(position == 7, from_above, 0.0) + jnp.where(position == 0, from_below, 0.0)


def single_component(field_values, geometry):
    total_x, total_y, total_z = field_values.shape
    zblock = math.gcd(total_z, 1024)
    block_count = total_z // zblock
    field_blocks = jnp.moveaxis(field_values.reshape(total_x, total_y, block_count, zblock), 2, 0)
    geometries = jnp.moveaxis(geometry.reshape(6, geometry.shape[1], geometry.shape[2], block_count, zblock // 8), 3, 0)
    local_terms = lax.map(lambda operands: stiffness(operands[0], operands[1]), (field_blocks, geometries))
    local_terms = jnp.moveaxis(local_terms, 0, 2).reshape(field_values.shape)
    summed = local_terms
    for direction in range(3):
        plane_extents = list(summed.shape)
        plane_extents[direction] = 1
        zero_plane = jnp.zeros(plane_extents, jnp.float32)
        summed = combine(summed, zero_plane, zero_plane, direction)
    return summed


def reference(nodal_scalar_values, geometry):
    return jnp.stack([single_component(nodal_scalar_values[component], geometry) for component in range(COMPONENTS)])
```

```python
import functools

import jax
import jax.numpy as jnp
import numpy as np
from jax import lax
from jax.experimental import pallas as pl
from jax.experimental.pallas import tpu as pltpu
from jax.sharding import PartitionSpec as P

interior_points = [
    -0.8717401485096066,
    -0.5917001814331423,
    -0.2092992179024789,
    0.2092992179024789,
    0.5917001814331423,
    0.8717401485096066,
]
MESH = pl.DeviceIdType.MESH
STEP = 256
LANES = 128


def legendre_seven(point):
    previous = 1.0
    current = point
    for order in range(1, 7):
        following = ((2 * order + 1) * point * current - order * previous) / (order + 1)
        previous = current
        current = following
    return current


def gll_tables():
    degree = 7
    points = [-1.0] + interior_points + [1.0]
    values = [legendre_seven(point) for point in points]
    node_count = degree + 1
    weights = np.array([2.0 / (degree * (degree + 1) * value * value) for value in values])
    derivative = np.zeros((node_count, node_count))
    for row_index in range(node_count):
        for col_index in range(node_count):
            if row_index != col_index:
                derivative[row_index, col_index] = values[row_index] / (
                    values[col_index] * (points[row_index] - points[col_index])
                )
    derivative[0, 0] = -degree * (degree + 1) / 4.0
    derivative[node_count - 1, node_count - 1] = degree * (degree + 1) / 4.0
    return (derivative, weights)


def halves(table):
    table = np.asarray(table, np.float32)
    high = table.astype(jnp.bfloat16)
    low = (table - high.astype(np.float32)).astype(jnp.bfloat16)
    return high, low


def tables():
    derivative, weights = gll_tables()
    eye = np.eye(8)
    plane_weight = np.kron(weights, weights)
    forward_xy = np.concatenate([np.kron(derivative, eye), np.kron(eye, derivative)], axis=0)
    back_xy = np.concatenate([np.kron(derivative.T, eye), np.kron(eye, derivative.T)], axis=1)
    back_xy = back_xy * np.tile(plane_weight, 2)[None, :]
    forward_z = np.kron(np.eye(16), derivative.T)
    back_z = np.kron(np.eye(16), derivative)
    high, low = halves(forward_xy)
    forward_xy = np.concatenate([high, high, low, low], axis=1)
    high, low = halves(back_xy)
    back_xy = np.concatenate(
        [np.concatenate([high, high], axis=1), np.concatenate([low, low], axis=1)], axis=0
    )
    high, low = halves(forward_z)
    forward_z = np.tile(np.concatenate([high, low], axis=1), (2, 1))
    high, low = halves(back_z)
    back_z = np.tile(np.concatenate([high, low], axis=1), (2, 1))
    matrices = np.concatenate([forward_xy, back_xy, forward_z, back_z], axis=0)
    plane = np.repeat(plane_weight[:, None], LANES, axis=1)
    along = np.repeat(np.tile(weights, LANES // 8)[None, :], 8, axis=0)
    scales = np.concatenate([plane, along], axis=0).astype(np.float32)
    return matrices, scales


def split(value):
    high = value.astype(jnp.bfloat16)
    low = (value - high.astype(jnp.float32)).astype(jnp.bfloat16)
    return high, low


def product(left, right):
    return jnp.dot(left, right, preferred_element_type=jnp.float32)


def along_lanes(high, low, table):
    pieces = []
    for start in range(0, high.shape[1], LANES):
        both = jnp.concatenate(
            [high[:, start : start + LANES], low[:, start : start + LANES]], axis=1
        )
        twice = product(both, table)
        pieces.append(twice[:, :LANES] + twice[:, LANES:])
    return jnp.concatenate(pieces, axis=1)


def kernel(
    sizes,
    chunk,
    u_hbm,
    geo_hbm,
    mat_hbm,
    scale_hbm,
    out,
    u,
    geo,
    mat,
    scale,
    metric,
    local,
    y_out,
    x_in,
    y_in,
    corner_out,
    corner_in,
    z_out,
    z_in,
    in_sem,
    const_sem,
    x_send,
    x_recv,
    y_send,
    y_recv,
    c_send,
    c_recv,
    z_send,
    z_recv,
):
    comps, _, _, total = u.shape
    count = total // chunk
    order = [0] + ([count - 1] if count > 1 else []) + list(range(1, count - 1))
    names = ("gx", "gy", "gz")
    place = {name: lax.axis_index(name) for name in names}
    below = {name: place[name] > 0 for name in names}
    above = {name: place[name] < sizes[name] - 1 for name in names}

    const_copies = [
        pltpu.make_async_copy(mat_hbm, mat, const_sem.at[0]),
        pltpu.make_async_copy(scale_hbm, scale, const_sem.at[1]),
        pltpu.make_async_copy(geo_hbm, geo, const_sem.at[2]),
    ]
    for copy in const_copies:
        copy.start()
    in_copies = {}
    for c in order:
        span = pl.ds(c * chunk, chunk)
        in_copies[c] = pltpu.make_async_copy(
            u_hbm.at[:, :, :, span], u.at[:, :, :, span], in_sem.at[c]
        )
        in_copies[c].start()

    barrier = pltpu.get_barrier_semaphore()
    for name in names:
        for there, by in ((below[name], -1), (above[name], 1)):

            @pl.when(there)
            def _(name=name, by=by):
                pl.semaphore_signal(
                    barrier, inc=1, device_id={name: place[name] + by}, device_id_type=MESH
                )

    for side in range(2):
        there = below if side == 0 else above

        @pl.when(jnp.logical_not(there["gx"]))
        def _(side=side):
            x_in[side] = jnp.zeros(x_in.shape[1:], jnp.float32)

        @pl.when(jnp.logical_not(there["gy"]))
        def _(side=side):
            y_in[side] = jnp.zeros(y_in.shape[1:], jnp.float32)
            corner_in[side] = jnp.zeros(corner_in.shape[1:], jnp.float32)

        @pl.when(jnp.logical_not(there["gz"]))
        def _(side=side):
            z_in[side] = jnp.zeros(z_in.shape[1:], jnp.float32)

    for copy in const_copies:
        copy.wait()

    rows = jnp.concatenate(
        [geo[k, 0] for k in range(6)] + [jnp.zeros((2, geo.shape[-1]), jnp.float32)], axis=0
    )
    lane = lax.broadcasted_iota(jnp.int32, (8, LANES), 1)
    for tile in range(total // LANES):
        first = tile * (LANES // 8)
        block = rows[:, first // LANES * LANES : first // LANES * LANES + LANES]
        spread = jnp.take_along_axis(block, lane // 8 + first % LANES, axis=1)
        metric[:, tile * LANES : (tile + 1) * LANES] = spread * scale[64:72, :]

    def x_copy(side, c):
        span = pl.ds(c * chunk, chunk)
        return pltpu.make_async_remote_copy(
            local.at[:, 7 if side == 0 else 0, :, span],
            x_in.at[side, :, :, span],
            x_send.at[side, c],
            x_recv.at[side, c],
            device_id={"gx": place["gx"] + (1 if side == 0 else -1)},
            device_id_type=MESH,
        )

    def y_copy(side, c):
        span = pl.ds(c * chunk, chunk)
        return pltpu.make_async_remote_copy(
            y_out.at[side, :, :, span],
            y_in.at[side, :, :, span],
            y_send.at[side, c],
            y_recv.at[side, c],
            device_id={"gy": place["gy"] + (1 if side == 0 else -1)},
            device_id_type=MESH,
        )

    def c_copy(side, c):
        span = pl.ds(c * chunk, chunk)
        return pltpu.make_async_remote_copy(
            corner_out.at[side, :, span],
            corner_in.at[side, :, span],
            c_send.at[side, c],
            c_recv.at[side, c],
            device_id={"gy": place["gy"] + (1 if side == 0 else -1)},
            device_id_type=MESH,
        )

    def z_copy(side):
        return pltpu.make_async_remote_copy(
            z_out.at[side],
            z_in.at[side],
            z_send.at[side],
            z_recv.at[side],
            device_id={"gz": place["gz"] + (1 if side == 0 else -1)},
            device_id_type=MESH,
        )

    def target(name, side):
        return above[name] if side == 0 else below[name]

    def source(name, side):
        return below[name] if side == 0 else above[name]

    def when_do(condition, act):
        @pl.when(condition)
        def _():
            act()

    forward_xy, back_xy = mat[0:128, :], mat[128:256, :]
    forward_z, back_z = mat[256:512, :], mat[512:768, :]

    greeted = sum(side[name].astype(jnp.int32) for name in names for side in (below, above))
    for at, c in enumerate(order):
        in_copies[c].wait()
        for start in range(c * chunk, (c + 1) * chunk, STEP):
            lanes = slice(start, start + STEP)
            g00, g11, g22, g01, g02, g12 = [metric[k : k + 1, lanes] for k in range(6)]
            for comp in range(comps):
                field = u[comp, :, :, lanes].reshape(64, STEP)
                high, low = split(field)
                both = product(forward_xy, jnp.concatenate([high, low, high, low], axis=0))
                grad_x, grad_y = both[:64], both[64:]
                grad_z = along_lanes(high, low, forward_z)
                flux_x = g00 * grad_x + g01 * grad_y + g02 * grad_z
                flux_y = g01 * grad_x + g11 * grad_y + g12 * grad_z
                flux_z = g02 * grad_x + g12 * grad_y + g22 * grad_z
                x_high, x_low = split(flux_x)
                y_high, y_low = split(flux_y)
                z_high, z_low = split(flux_z)
                twice = product(back_xy, jnp.concatenate([x_high, y_high, x_low, y_low], axis=0))
                terms = twice[:64] + twice[64:]
                weight = jnp.concatenate([scale[0:64, :]] * (STEP // LANES), axis=1)
                terms = terms + weight * along_lanes(z_high, z_low, back_z)
                terms = terms.reshape(8, 8, STEP)
                local[comp, :, :, lanes] = terms
                for n in range(8):
                    y_out[0, comp, n : n + 1, lanes] = terms[n, 7:8]
                    y_out[1, comp, n : n + 1, lanes] = terms[n, 0:1]
        if at == 0:
            pl.semaphore_wait(barrier, greeted)
        for side in range(2):
            when_do(target("gx", side), lambda: x_copy(side, c).start())
            when_do(target("gy", side), lambda: y_copy(side, c).start())

    for c in order:
        lanes = slice(c * chunk, (c + 1) * chunk)
        for side in range(2):
            when_do(source("gx", side), lambda: x_copy(side, c).wait_recv())
        for side in range(2):
            row = 7 if side == 0 else 0
            for comp in range(comps):
                for x_side in range(2):
                    at_row = 2 * comp + x_side
                    corner_out[side, at_row : at_row + 1, lanes] = x_in[
                        x_side, comp, row : row + 1, lanes
                    ]
            when_do(target("gy", side), lambda: c_copy(side, c).start())

    sub = lax.broadcasted_iota(jnp.int32, (8, LANES), 0)

    def xy_sum(comp, n, lanes):
        value = local[comp, n, :, lanes]
        from_below = y_in[0, comp, n : n + 1, lanes]
        from_above = y_in[1, comp, n : n + 1, lanes]
        if n in (0, 7):
            x_side = 0 if n == 0 else 1
            at_row = 2 * comp + x_side
            value = value + x_in[x_side, comp, :, lanes]
            from_below = from_below + corner_in[0, at_row : at_row + 1, lanes]
            from_above = from_above + corner_in[1, at_row : at_row + 1, lanes]
        where = lax.broadcasted_iota(jnp.int32, value.shape, 0)
        value = value + jnp.where(where == 0, from_below, 0.0)
        return value + jnp.where(where == 7, from_above, 0.0)

    def arrived(c):
        for side in range(2):
            when_do(source("gy", side), lambda: y_copy(side, c).wait_recv())
            when_do(source("gy", side), lambda: c_copy(side, c).wait_recv())

    edge = order[:2] if count > 1 else order
    for c in edge:
        arrived(c)
    for side in range(2):
        lanes = slice(total - LANES, total) if side == 0 else slice(0, LANES)
        for comp in range(comps):
            for n in range(8):
                z_out[side, comp, n] = xy_sum(comp, n, lanes)
        when_do(target("gz", side), lambda: z_copy(side).start())

    for c in order[len(edge) :]:
        arrived(c)
    for side in range(2):
        when_do(source("gz", side), lambda: z_copy(side).wait_recv())

    for comp in range(comps):
        for n in range(8):
            value = xy_sum(comp, n, slice(0, total))
            left = jnp.concatenate(
                [z_in[0, comp, n], value, z_in[1, comp, n]], axis=1
            )
            width = left.shape[1]
            before = pltpu.roll(left, 1, 1)[:, LANES : LANES + total]
            after = pltpu.roll(left, width - 1, 1)[:, LANES : LANES + total]
            position = lax.broadcasted_iota(jnp.int32, value.shape, 1) % 8
            extra = jnp.where(position == 7, after, jnp.where(position == 0, before, 0.0))
            out[comp, n] = value + extra

    for c in order:
        for side in range(2):
            when_do(target("gx", side), lambda: x_copy(side, c).wait_send())
            when_do(target("gy", side), lambda: y_copy(side, c).wait_send())
            when_do(target("gy", side), lambda: c_copy(side, c).wait_send())
    for side in range(2):
        when_do(target("gz", side), lambda: z_copy(side).wait_send())


def local_part(sizes, nodal_scalar_values, geometry):
    comps, _, _, total = nodal_scalar_values.shape
    chunk = min(512, total)
    count = total // chunk
    matrices, scales = tables()
    f32 = jnp.float32
    dma = pltpu.SemaphoreType.DMA
    any_space = pl.BlockSpec(memory_space=pl.ANY)
    return pl.pallas_call(
        functools.partial(kernel, sizes, chunk),
        out_shape=jax.ShapeDtypeStruct(nodal_scalar_values.shape, f32),
        in_specs=[any_space] * 4,
        out_specs=pl.BlockSpec(memory_space=pltpu.VMEM),
        scratch_shapes=[
            pltpu.VMEM(nodal_scalar_values.shape, f32),
            pltpu.VMEM(geometry.shape, f32),
            pltpu.VMEM(matrices.shape, jnp.bfloat16),
            pltpu.VMEM(scales.shape, f32),
            pltpu.VMEM((8, total), f32),
            pltpu.VMEM(nodal_scalar_values.shape, f32),
            pltpu.VMEM((2, comps, 8, total), f32),
            pltpu.VMEM((2, comps, 8, total), f32),
            pltpu.VMEM((2, comps, 8, total), f32),
            pltpu.VMEM((2, 8, total), f32),
            pltpu.VMEM((2, 8, total), f32),
            pltpu.VMEM((2, comps, 8, 8, LANES), f32),
            pltpu.VMEM((2, comps, 8, 8, LANES), f32),
            dma((count,)),
            dma((3,)),
            dma((2, count)),
            dma((2, count)),
            dma((2, count)),
            dma((2, count)),
            dma((2, count)),
            dma((2, count)),
            dma((2,)),
            dma((2,)),
        ],
        compiler_params=pltpu.CompilerParams(collective_id=0, has_side_effects=True),
        name="poisson",
    )(nodal_scalar_values, geometry, jnp.asarray(matrices), jnp.asarray(scales))


def solution(mesh):
    return jax.shard_map(
        functools.partial(local_part, dict(mesh.shape)),
        mesh=mesh,
        in_specs=(P(None, "gx", "gy", "gz"), P(None, "gx", "gy", "gz")),
        out_specs=P(None, "gx", "gy", "gz"),
        check_vma=False,
    )
```

```python
import functools

import jax
import jax.numpy as jnp
import numpy as np
from jax import lax
from jax.experimental import pallas as pl
from jax.experimental.pallas import tpu as pltpu
from jax.sharding import PartitionSpec as P

interior_points = [
    -0.8717401485096066,
    -0.5917001814331423,
    -0.2092992179024789,
    0.2092992179024789,
    0.5917001814331423,
    0.8717401485096066,
]
MESH = pl.DeviceIdType.MESH
STEP = 256
LANES = 128
X_FIRST = True
LAG = 4


def legendre_seven(point):
    previous = 1.0
    current = point
    for order in range(1, 7):
        following = ((2 * order + 1) * point * current - order * previous) / (order + 1)
        previous = current
        current = following
    return current


def gll_tables():
    degree = 7
    points = [-1.0] + interior_points + [1.0]
    values = [legendre_seven(point) for point in points]
    node_count = degree + 1
    weights = np.array([2.0 / (degree * (degree + 1) * value * value) for value in values])
    derivative = np.zeros((node_count, node_count))
    for row_index in range(node_count):
        for col_index in range(node_count):
            if row_index != col_index:
                derivative[row_index, col_index] = values[row_index] / (
                    values[col_index] * (points[row_index] - points[col_index])
                )
    derivative[0, 0] = -degree * (degree + 1) / 4.0
    derivative[node_count - 1, node_count - 1] = degree * (degree + 1) / 4.0
    return (derivative, weights)


def halves(table):
    table = np.asarray(table, np.float32)
    high = table.astype(jnp.bfloat16)
    low = (table - high.astype(np.float32)).astype(jnp.bfloat16)
    return high, low


def tables():
    derivative, weights = gll_tables()
    eye = np.eye(8)
    plane_weight = np.kron(weights, weights)
    forward_xy = np.concatenate([np.kron(derivative, eye), np.kron(eye, derivative)], axis=0)
    back_xy = np.concatenate([np.kron(derivative.T, eye), np.kron(eye, derivative.T)], axis=1)
    back_xy = back_xy * np.tile(plane_weight, 2)[None, :]
    forward_z = np.kron(np.eye(16), derivative.T)
    back_z = np.kron(np.eye(16), derivative)
    high, low = halves(forward_xy)
    forward_xy = np.concatenate([high, high, low, low], axis=1)
    high, low = halves(back_xy)
    back_xy = np.concatenate(
        [np.concatenate([high, high], axis=1), np.concatenate([low, low], axis=1)], axis=0
    )
    high, low = halves(forward_z)
    forward_z = np.tile(np.concatenate([high, low], axis=1), (2, 1))
    high, low = halves(back_z)
    back_z = np.tile(np.concatenate([high, low], axis=1), (2, 1))
    matrices = np.concatenate([forward_xy, back_xy, forward_z, back_z], axis=0)
    plane = np.repeat(plane_weight[:, None], LANES, axis=1)
    along = np.repeat(np.tile(weights, LANES // 8)[None, :], 8, axis=0)
    scales = np.concatenate([plane, along], axis=0).astype(np.float32)
    return matrices, scales


def seat(comp, m):
    if m in (0, 7):
        return 0, 2 * comp + (1 if m == 7 else 0)
    if comp:
        return comp, m - 1
    return (m - 1) // 2, 6 + (m - 1) % 2


def split(value):
    high = value.astype(jnp.bfloat16)
    low = (value - high.astype(jnp.float32)).astype(jnp.bfloat16)
    return high, low


def product(left, right):
    return jnp.dot(left, right, preferred_element_type=jnp.float32)


def along_lanes(high, low, table):
    pieces = []
    for start in range(0, high.shape[1], LANES):
        both = jnp.concatenate(
            [high[:, start : start + LANES], low[:, start : start + LANES]], axis=1
        )
        twice = product(both, table)
        pieces.append(twice[:, :LANES] + twice[:, LANES:])
    return jnp.concatenate(pieces, axis=1)


def kernel(
    sizes,
    chunk,
    u_hbm,
    geo_hbm,
    mat_hbm,
    scale_hbm,
    out,
    u,
    geo,
    mat,
    scale,
    metric,
    local,
    x_out,
    y_out,
    x_in,
    y_in,
    corner_out,
    corner_in,
    z_out,
    z_in,
    relay,
    in_sem,
    const_sem,
    x_send,
    x_recv,
    y_send,
    y_recv,
    c_send,
    c_recv,
    z_send,
    z_recv,
    r_send,
    r_recv,
    b_send,
    b_recv,
):
    comps, _, _, total = u.shape
    count = total // chunk
    order = [0] + ([count - 1] if count > 1 else []) + list(range(1, count - 1))
    names = ("gx", "gy", "gz")
    place = {name: lax.axis_index(name) for name in names}
    below = {name: place[name] > 0 for name in names}
    above = {name: place[name] < sizes[name] - 1 for name in names}

    const_copies = [
        pltpu.make_async_copy(mat_hbm, mat, const_sem.at[0]),
        pltpu.make_async_copy(scale_hbm, scale, const_sem.at[1]),
        pltpu.make_async_copy(geo_hbm, geo, const_sem.at[2]),
    ]
    for copy in const_copies:
        copy.start()
    in_copies = {}
    for c in order:
        span = pl.ds(c * chunk, chunk)
        in_copies[c] = pltpu.make_async_copy(
            u_hbm.at[:, :, :, span], u.at[:, :, :, span], in_sem.at[c]
        )
        in_copies[c].start()

    barrier = pltpu.get_barrier_semaphore()
    for name in names:
        for there, by in ((below[name], -1), (above[name], 1)):

            @pl.when(there)
            def _(name=name, by=by):
                pl.semaphore_signal(
                    barrier, inc=1, device_id={name: place[name] + by}, device_id_type=MESH
                )

    detour = sizes["gx"] == 4
    relayed = order[: count * 3 // 4] if detour else []
    opposite = lax.rem(place["gx"] + 2, 4)
    if detour:
        pl.semaphore_signal(barrier, inc=1, device_id={"gx": opposite}, device_id_type=MESH)

    for side in range(2):
        there = below if side == 0 else above

        @pl.when(jnp.logical_not(there["gx"]))
        def _(side=side):
            x_in[side] = jnp.zeros(x_in.shape[1:], jnp.float32)

        @pl.when(jnp.logical_not(there["gy"]))
        def _(side=side):
            y_in[side] = jnp.zeros(y_in.shape[1:], jnp.float32)
            corner_in[side] = jnp.zeros(corner_in.shape[1:], jnp.float32)

        @pl.when(jnp.logical_not(there["gz"]))
        def _(side=side):
            z_in[side] = jnp.zeros(z_in.shape[1:], jnp.float32)

    for copy in const_copies:
        copy.wait()

    rows = jnp.concatenate(
        [geo[k, 0] for k in range(6)] + [jnp.zeros((2, geo.shape[-1]), jnp.float32)], axis=0
    )
    lane = lax.broadcasted_iota(jnp.int32, (8, LANES), 1)
    for tile in range(total // LANES):
        first = tile * (LANES // 8)
        block = rows[:, first // LANES * LANES : first // LANES * LANES + LANES]
        spread = jnp.take_along_axis(block, lane // 8 + first % LANES, axis=1)
        metric[:, tile * LANES : (tile + 1) * LANES] = spread * scale[64:72, :]

    def x_copy(side, c):
        span = pl.ds(c * chunk, chunk)
        return pltpu.make_async_remote_copy(
            x_out.at[side, 0, :, span],
            x_in.at[side, 0, :, span],
            x_send.at[side, c],
            x_recv.at[side, c],
            device_id={"gx": place["gx"] + (1 if side == 0 else -1)},
            device_id_type=MESH,
        )

    def bulk_copy(side, c):
        span = pl.ds(c * chunk, chunk)
        return pltpu.make_async_remote_copy(
            x_out.at[side, 1:, :, span],
            x_in.at[side, 1:, :, span],
            b_send.at[side, c],
            b_recv.at[side, c],
            device_id={"gx": place["gx"] + (1 if side == 0 else -1)},
            device_id_type=MESH,
        )

    def middle(side):
        return place["gx"] == 1 + side

    def by_way_of(side):
        return 3 * (1 - side) if X_FIRST else 3 * side

    def hop_copy(side, c):
        span = pl.ds(c * chunk, chunk)
        return pltpu.make_async_remote_copy(
            x_out.at[side, 1:, :, span],
            relay.at[:, :, span],
            b_send.at[side, c],
            r_recv.at[c],
            device_id={"gx": by_way_of(side)},
            device_id_type=MESH,
        )

    def onward_copy(side, c):
        span = pl.ds(c * chunk, chunk)
        return pltpu.make_async_remote_copy(
            relay.at[:, :, span],
            x_in.at[side, 1:, :, span],
            r_send.at[c],
            b_recv.at[side, c],
            device_id={"gx": 2 - side},
            device_id_type=MESH,
        )

    def forward(c):
        for side in range(2):

            @pl.when(place["gx"] == by_way_of(side))
            def _(side=side):
                hop_copy(side, c).wait_recv()
                onward_copy(side, c).start()

    def send_bulk(c):
        for side in range(2):
            if c in relayed:
                straight = jnp.logical_and(target("gx", side), jnp.logical_not(middle(side)))
                when_do(straight, lambda: bulk_copy(side, c).start())
                when_do(middle(side), lambda: hop_copy(side, c).start())
            else:
                when_do(target("gx", side), lambda: bulk_copy(side, c).start())

    def y_copy(side, c):
        span = pl.ds(c * chunk, chunk)
        return pltpu.make_async_remote_copy(
            y_out.at[side, :, :, span],
            y_in.at[side, :, :, span],
            y_send.at[side, c],
            y_recv.at[side, c],
            device_id={"gy": place["gy"] + (1 if side == 0 else -1)},
            device_id_type=MESH,
        )

    def c_copy(side, c):
        span = pl.ds(c * chunk, chunk)
        return pltpu.make_async_remote_copy(
            corner_out.at[side, :, span],
            corner_in.at[side, :, span],
            c_send.at[side, c],
            c_recv.at[side, c],
            device_id={"gy": place["gy"] + (1 if side == 0 else -1)},
            device_id_type=MESH,
        )

    def z_copy(side):
        return pltpu.make_async_remote_copy(
            z_out.at[side],
            z_in.at[side],
            z_send.at[side],
            z_recv.at[side],
            device_id={"gz": place["gz"] + (1 if side == 0 else -1)},
            device_id_type=MESH,
        )

    def target(name, side):
        return above[name] if side == 0 else below[name]

    def source(name, side):
        return below[name] if side == 0 else above[name]

    def when_do(condition, act):
        @pl.when(condition)
        def _():
            act()

    def corners(c):
        lanes = slice(c * chunk, (c + 1) * chunk)
        for side in range(2):
            when_do(source("gx", side), lambda: x_copy(side, c).wait_recv())
        for side in range(2):
            for comp in range(comps):
                for x_side in range(2):
                    at_row = 2 * comp + x_side
                    tile, row = seat(comp, 7 if side == 0 else 0)
                    corner_out[side, at_row : at_row + 1, lanes] = x_in[
                        x_side, tile, row : row + 1, lanes
                    ]
            when_do(target("gy", side), lambda: c_copy(side, c).start())

    forward_xy, back_xy = mat[0:128, :], mat[128:256, :]
    forward_z, back_z = mat[256:512, :], mat[512:768, :]

    greeted = sum(side[name].astype(jnp.int32) for name in names for side in (below, above))
    greeted = greeted + (1 if detour else 0)
    waiting, cornering = list(relayed), list(order)
    for at, c in enumerate(order):
        in_copies[c].wait()
        for start in range(c * chunk, (c + 1) * chunk, STEP):
            lanes = slice(start, start + STEP)
            g00, g11, g22, g01, g02, g12 = [metric[k : k + 1, lanes] for k in range(6)]
            for comp in range(comps):
                field = u[comp, :, :, lanes].reshape(64, STEP)
                high, low = split(field)
                both = product(forward_xy, jnp.concatenate([high, low, high, low], axis=0))
                grad_x, grad_y = both[:64], both[64:]
                grad_z = along_lanes(high, low, forward_z)
                flux_x = g00 * grad_x + g01 * grad_y + g02 * grad_z
                flux_y = g01 * grad_x + g11 * grad_y + g12 * grad_z
                flux_z = g02 * grad_x + g12 * grad_y + g22 * grad_z
                x_high, x_low = split(flux_x)
                y_high, y_low = split(flux_y)
                z_high, z_low = split(flux_z)
                twice = product(back_xy, jnp.concatenate([x_high, y_high, x_low, y_low], axis=0))
                terms = twice[:64] + twice[64:]
                weight = jnp.concatenate([scale[0:64, :]] * (STEP // LANES), axis=1)
                terms = terms + weight * along_lanes(z_high, z_low, back_z)
                terms = terms.reshape(8, 8, STEP)
                local[comp, :, :, lanes] = terms
                for n in range(8):
                    y_out[0, comp, n : n + 1, lanes] = terms[n, 7:8]
                    y_out[1, comp, n : n + 1, lanes] = terms[n, 0:1]
                    tile, row = seat(comp, n)
                    x_out[0, tile, row : row + 1, lanes] = terms[7, n : n + 1]
                    x_out[1, tile, row : row + 1, lanes] = terms[0, n : n + 1]
        if at == 0:
            pl.semaphore_wait(barrier, greeted)
        for side in range(2):
            when_do(target("gx", side), lambda: x_copy(side, c).start())
            when_do(target("gy", side), lambda: y_copy(side, c).start())
        if at:
            send_bulk(order[at - 1])
        if at >= LAG and cornering:
            corners(cornering.pop(0))
        if at >= LAG + 1 and waiting:
            forward(waiting.pop(0))
    send_bulk(order[-1])
    while waiting or cornering:
        if cornering:
            corners(cornering.pop(0))
        if waiting:
            forward(waiting.pop(0))

    def xy_sum(comp, n, lanes):
        value = local[comp, n, :, lanes]
        from_below = y_in[0, comp, n : n + 1, lanes]
        from_above = y_in[1, comp, n : n + 1, lanes]
        if n in (0, 7):
            x_side = 0 if n == 0 else 1
            at_row = 2 * comp + x_side
            seats = [seat(comp, m) for m in range(8)]
            rows = [x_in[x_side, tile, row : row + 1, lanes] for tile, row in seats]
            value = value + jnp.concatenate(rows, axis=0)
            from_below = from_below + corner_in[0, at_row : at_row + 1, lanes]
            from_above = from_above + corner_in[1, at_row : at_row + 1, lanes]
        where = lax.broadcasted_iota(jnp.int32, value.shape, 0)
        value = value + jnp.where(where == 0, from_below, 0.0)
        return value + jnp.where(where == 7, from_above, 0.0)

    def arrived(c):
        for side in range(2):
            when_do(source("gx", side), lambda: bulk_copy(side, c).wait_recv())
            when_do(source("gy", side), lambda: y_copy(side, c).wait_recv())
            when_do(source("gy", side), lambda: c_copy(side, c).wait_recv())

    def finish(first, last):
        for comp in range(comps):
            for n in range(8):
                value = xy_sum(comp, n, slice(max(first - LANES, 0), min(last + LANES, total)))
                if first == 0:
                    value = jnp.concatenate([z_in[0, comp, n], value], axis=1)
                if last == total:
                    value = jnp.concatenate([value, z_in[1, comp, n]], axis=1)
                width = value.shape[1]
                before = pltpu.roll(value, 1, 1)[:, LANES:-LANES]
                after = pltpu.roll(value, width - 1, 1)[:, LANES:-LANES]
                position = lax.broadcasted_iota(jnp.int32, before.shape, 1) % 8
                extra = jnp.where(position == 7, after, jnp.where(position == 0, before, 0.0))
                out[comp, n, :, first:last] = value[:, LANES:-LANES] + extra

    edge = order[:2] if count > 1 else order
    group = min(2 * chunk, total)
    groups = list(range(total // group))
    here = set()
    z_here = False
    for at, c in enumerate(order):
        arrived(c)
        here.add(c)
        if at == len(edge) - 1:
            for side in range(2):
                lanes = slice(total - LANES, total) if side == 0 else slice(0, LANES)
                for comp in range(comps):
                    for n in range(8):
                        z_out[side, comp, n] = xy_sum(comp, n, lanes)
                when_do(target("gz", side), lambda: z_copy(side).start())
        for g in list(groups):
            first, last = g * group // chunk, (g + 1) * group // chunk
            if all(i in here for i in range(max(first - 1, 0), min(last + 1, count))):
                groups.remove(g)
                ends = g * group, (g + 1) * group
                if not z_here and (ends[0] == 0 or ends[1] == total):
                    z_here = True
                    for side in range(2):
                        when_do(source("gz", side), lambda: z_copy(side).wait_recv())
                finish(*ends)

    for c in order:
        for side in range(2):
            when_do(target("gx", side), lambda: x_copy(side, c).wait_send())
            when_do(target("gx", side), lambda: bulk_copy(side, c).wait_send())
            when_do(target("gy", side), lambda: y_copy(side, c).wait_send())
            when_do(target("gy", side), lambda: c_copy(side, c).wait_send())
    for side in range(2):
        when_do(target("gz", side), lambda: z_copy(side).wait_send())
        for c in relayed:
            when_do(place["gx"] == by_way_of(side), lambda: onward_copy(side, c).wait_send())


def local_part(sizes, nodal_scalar_values, geometry):
    comps, _, _, total = nodal_scalar_values.shape
    chunk = min(256, total)
    count = total // chunk
    matrices, scales = tables()
    f32 = jnp.float32
    dma = pltpu.SemaphoreType.DMA
    any_space = pl.BlockSpec(memory_space=pl.ANY)
    return pl.pallas_call(
        functools.partial(kernel, sizes, chunk),
        out_shape=pltpu.VMEM(nodal_scalar_values.shape, f32),
        in_specs=[any_space] * 4,
        out_specs=pl.BlockSpec(memory_space=pltpu.VMEM),
        scratch_shapes=[
            pltpu.VMEM(nodal_scalar_values.shape, f32),
            pltpu.VMEM(geometry.shape, f32),
            pltpu.VMEM(matrices.shape, jnp.bfloat16),
            pltpu.VMEM(scales.shape, f32),
            pltpu.VMEM((8, total), f32),
            pltpu.VMEM(nodal_scalar_values.shape, f32),
            pltpu.VMEM((2, comps, 8, total), f32),
            pltpu.VMEM((2, comps, 8, total), f32),
            pltpu.VMEM((2, comps, 8, total), f32),
            pltpu.VMEM((2, comps, 8, total), f32),
            pltpu.VMEM((2, 8, total), f32),
            pltpu.VMEM((2, 8, total), f32),
            pltpu.VMEM((2, comps, 8, 8, LANES), f32),
            pltpu.VMEM((2, comps, 8, 8, LANES), f32),
            pltpu.VMEM((comps - 1, 8, total), f32),
            dma((count,)),
            dma((3,)),
            dma((2, count)),
            dma((2, count)),
            dma((2, count)),
            dma((2, count)),
            dma((2, count)),
            dma((2, count)),
            dma((2,)),
            dma((2,)),
            dma((count,)),
            dma((count,)),
            dma((2, count)),
            dma((2, count)),
        ],
        compiler_params=pltpu.CompilerParams(collective_id=0, has_side_effects=True),
        name="poisson",
    )(nodal_scalar_values, geometry, jnp.asarray(matrices), jnp.asarray(scales))


def solution(mesh):
    return jax.shard_map(
        functools.partial(local_part, dict(mesh.shape)),
        mesh=mesh,
        in_specs=(P(None, "gx", "gy", "gz"), P(None, "gx", "gy", "gz")),
        out_specs=P(None, "gx", "gy", "gz"),
        check_vma=False,
    )
```

```python
import functools

import jax
import jax.numpy as jnp
import numpy as np
from jax import lax
from jax.experimental import pallas as pl
from jax.experimental.pallas import tpu as pltpu
from jax.sharding import PartitionSpec as P

interior_points = [
    -0.8717401485096066,
    -0.5917001814331423,
    -0.2092992179024789,
    0.2092992179024789,
    0.5917001814331423,
    0.8717401485096066,
]
MESH = pl.DeviceIdType.MESH
STEP = 256
LANES = 128
X_FIRST = True
LAG = 5


def legendre_seven(point):
    previous = 1.0
    current = point
    for order in range(1, 7):
        following = ((2 * order + 1) * point * current - order * previous) / (order + 1)
        previous = current
        current = following
    return current


def gll_tables():
    degree = 7
    points = [-1.0] + interior_points + [1.0]
    values = [legendre_seven(point) for point in points]
    node_count = degree + 1
    weights = np.array([2.0 / (degree * (degree + 1) * value * value) for value in values])
    derivative = np.zeros((node_count, node_count))
    for row_index in range(node_count):
        for col_index in range(node_count):
            if row_index != col_index:
                derivative[row_index, col_index] = values[row_index] / (
                    values[col_index] * (points[row_index] - points[col_index])
                )
    derivative[0, 0] = -degree * (degree + 1) / 4.0
    derivative[node_count - 1, node_count - 1] = degree * (degree + 1) / 4.0
    return (derivative, weights)


def halves(table):
    table = np.asarray(table, np.float32)
    high = table.astype(jnp.bfloat16)
    low = (table - high.astype(np.float32)).astype(jnp.bfloat16)
    return high, low


def tables():
    derivative, weights = gll_tables()
    eye = np.eye(8)
    plane_weight = np.kron(weights, weights)
    forward_xy = np.concatenate([np.kron(derivative, eye), np.kron(eye, derivative)], axis=0)
    back_xy = np.concatenate([np.kron(derivative.T, eye), np.kron(eye, derivative.T)], axis=1)
    back_xy = back_xy * np.tile(plane_weight, 2)[None, :]
    forward_z = np.kron(np.eye(16), derivative.T)
    back_z = np.kron(np.eye(16), derivative)
    high, low = halves(forward_xy)
    forward_xy = np.concatenate([high, high, low, low], axis=1)
    high, low = halves(back_xy)
    back_xy = np.concatenate(
        [np.concatenate([high, high], axis=1), np.concatenate([low, low], axis=1)], axis=0
    )
    high, low = halves(forward_z)
    forward_z = np.tile(np.concatenate([high, low], axis=1), (2, 1))
    high, low = halves(back_z)
    back_z = np.tile(np.concatenate([high, low], axis=1), (2, 1))
    matrices = np.concatenate([forward_xy, back_xy, forward_z, back_z], axis=0)
    plane = np.repeat(plane_weight[:, None], LANES, axis=1)
    along = np.repeat(np.tile(weights, LANES // 8)[None, :], 8, axis=0)
    scales = np.concatenate([plane, along], axis=0).astype(np.float32)
    return matrices, scales


def seat(comp, m):
    if m in (0, 7):
        return 0, 2 * comp + (1 if m == 7 else 0)
    if comp:
        return comp, m - 1
    return (m - 1) // 2, 6 + (m - 1) % 2


def split(value):
    high = value.astype(jnp.bfloat16)
    low = (value - high.astype(jnp.float32)).astype(jnp.bfloat16)
    return high, low


def product(left, right):
    return jnp.dot(left, right, preferred_element_type=jnp.float32)


def along_lanes(pairs, table):
    rows, width = pairs[0][0].shape
    spans = [slice(start, start + LANES) for start in range(0, width, LANES)]
    stacked = [
        jnp.concatenate([high[:, span], low[:, span]], axis=1)
        for high, low in pairs
        for span in spans
    ]
    twice = product(jnp.concatenate(stacked, axis=0), table)
    once = twice[:, :LANES] + twice[:, LANES:]
    pieces = [once[at * rows : (at + 1) * rows] for at in range(len(stacked))]
    return [
        jnp.concatenate(pieces[at : at + len(spans)], axis=1)
        for at in range(0, len(pieces), len(spans))
    ]


def kernel(
    sizes,
    chunk,
    u_hbm,
    geo_hbm,
    mat_hbm,
    scale_hbm,
    out,
    u,
    geo,
    mat,
    scale,
    metric,
    local,
    x_out,
    y_out,
    x_in,
    y_in,
    corner_out,
    corner_in,
    z_out,
    z_in,
    relay,
    in_sem,
    const_sem,
    x_send,
    x_recv,
    y_send,
    y_recv,
    c_send,
    c_recv,
    z_send,
    z_recv,
    r_send,
    r_recv,
    b_send,
    b_recv,
):
    comps, _, _, total = u.shape
    count = total // chunk
    order = [0] + ([count - 1] if count > 1 else []) + list(range(1, count - 1))
    names = ("gx", "gy", "gz")
    place = {name: lax.axis_index(name) for name in names}
    below = {name: place[name] > 0 for name in names}
    above = {name: place[name] < sizes[name] - 1 for name in names}

    const_copies = [
        pltpu.make_async_copy(mat_hbm, mat, const_sem.at[0]),
        pltpu.make_async_copy(scale_hbm, scale, const_sem.at[1]),
        pltpu.make_async_copy(geo_hbm, geo, const_sem.at[2]),
    ]
    for copy in const_copies:
        copy.start()
    in_copies = {}
    for c in order:
        span = pl.ds(c * chunk, chunk)
        in_copies[c] = pltpu.make_async_copy(
            u_hbm.at[:, :, :, span], u.at[:, :, :, span], in_sem.at[c]
        )
        in_copies[c].start()

    barrier = pltpu.get_barrier_semaphore()
    for name in names:
        for there, by in ((below[name], -1), (above[name], 1)):

            @pl.when(there)
            def _(name=name, by=by):
                pl.semaphore_signal(
                    barrier, inc=1, device_id={name: place[name] + by}, device_id_type=MESH
                )

    detour = sizes["gx"] == 4
    relayed = order[: count * 3 // 4] if detour else []
    opposite = lax.rem(place["gx"] + 2, 4)
    if detour:
        pl.semaphore_signal(barrier, inc=1, device_id={"gx": opposite}, device_id_type=MESH)

    for side in range(2):
        there = below if side == 0 else above

        @pl.when(jnp.logical_not(there["gx"]))
        def _(side=side):
            x_in[side] = jnp.zeros(x_in.shape[1:], jnp.float32)

        @pl.when(jnp.logical_not(there["gy"]))
        def _(side=side):
            y_in[side] = jnp.zeros(y_in.shape[1:], jnp.float32)
            corner_in[side] = jnp.zeros(corner_in.shape[1:], jnp.float32)

        @pl.when(jnp.logical_not(there["gz"]))
        def _(side=side):
            z_in[side] = jnp.zeros(z_in.shape[1:], jnp.float32)

    for copy in const_copies:
        copy.wait()

    rows = jnp.concatenate(
        [geo[k, 0] for k in range(6)] + [jnp.zeros((2, geo.shape[-1]), jnp.float32)], axis=0
    )
    lane = lax.broadcasted_iota(jnp.int32, (8, LANES), 1)
    for tile in range(total // LANES):
        first = tile * (LANES // 8)
        block = rows[:, first // LANES * LANES : first // LANES * LANES + LANES]
        spread = jnp.take_along_axis(block, lane // 8 + first % LANES, axis=1)
        metric[:, tile * LANES : (tile + 1) * LANES] = spread * scale[64:72, :]

    def x_copy(side, c):
        span = pl.ds(c * chunk, chunk)
        return pltpu.make_async_remote_copy(
            x_out.at[side, 0, :, span],
            x_in.at[side, 0, :, span],
            x_send.at[side, c],
            x_recv.at[side, c],
            device_id={"gx": place["gx"] + (1 if side == 0 else -1)},
            device_id_type=MESH,
        )

    def bulk_copy(side, c):
        span = pl.ds(c * chunk, chunk)
        return pltpu.make_async_remote_copy(
            x_out.at[side, 1:, :, span],
            x_in.at[side, 1:, :, span],
            b_send.at[side, c],
            b_recv.at[side, c],
            device_id={"gx": place["gx"] + (1 if side == 0 else -1)},
            device_id_type=MESH,
        )

    def middle(side):
        return place["gx"] == 1 + side

    def by_way_of(side):
        return 3 * (1 - side) if X_FIRST else 3 * side

    def hop_copy(side, c):
        span = pl.ds(c * chunk, chunk)
        return pltpu.make_async_remote_copy(
            x_out.at[side, 1:, :, span],
            relay.at[:, :, span],
            b_send.at[side, c],
            r_recv.at[c],
            device_id={"gx": by_way_of(side)},
            device_id_type=MESH,
        )

    def onward_copy(side, c):
        span = pl.ds(c * chunk, chunk)
        return pltpu.make_async_remote_copy(
            relay.at[:, :, span],
            x_in.at[side, 1:, :, span],
            r_send.at[c],
            b_recv.at[side, c],
            device_id={"gx": 2 - side},
            device_id_type=MESH,
        )

    def forward(c):
        for side in range(2):

            @pl.when(place["gx"] == by_way_of(side))
            def _(side=side):
                hop_copy(side, c).wait_recv()
                onward_copy(side, c).start()

    def send_bulk(c):
        for side in range(2):
            if c in relayed:
                straight = jnp.logical_and(target("gx", side), jnp.logical_not(middle(side)))
                when_do(straight, lambda: bulk_copy(side, c).start())
                when_do(middle(side), lambda: hop_copy(side, c).start())
            else:
                when_do(target("gx", side), lambda: bulk_copy(side, c).start())

    def y_copy(side, c):
        span = pl.ds(c * chunk, chunk)
        return pltpu.make_async_remote_copy(
            y_out.at[side, :, :, span],
            y_in.at[side, :, :, span],
            y_send.at[side, c],
            y_recv.at[side, c],
            device_id={"gy": place["gy"] + (1 if side == 0 else -1)},
            device_id_type=MESH,
        )

    def c_copy(side, c):
        span = pl.ds(c * chunk, chunk)
        return pltpu.make_async_remote_copy(
            corner_out.at[side, :, span],
            corner_in.at[side, :, span],
            c_send.at[side, c],
            c_recv.at[side, c],
            device_id={"gy": place["gy"] + (1 if side == 0 else -1)},
            device_id_type=MESH,
        )

    def z_copy(side):
        return pltpu.make_async_remote_copy(
            z_out.at[side],
            z_in.at[side],
            z_send.at[side],
            z_recv.at[side],
            device_id={"gz": place["gz"] + (1 if side == 0 else -1)},
            device_id_type=MESH,
        )

    def target(name, side):
        return above[name] if side == 0 else below[name]

    def source(name, side):
        return below[name] if side == 0 else above[name]

    def when_do(condition, act):
        @pl.when(condition)
        def _():
            act()

    def corners(c):
        lanes = slice(c * chunk, (c + 1) * chunk)
        for side in range(2):
            when_do(source("gx", side), lambda: x_copy(side, c).wait_recv())
        for side in range(2):
            for comp in range(comps):
                for x_side in range(2):
                    at_row = 2 * comp + x_side
                    tile, row = seat(comp, 7 if side == 0 else 0)
                    corner_out[side, at_row : at_row + 1, lanes] = x_in[
                        x_side, tile, row : row + 1, lanes
                    ]
            when_do(target("gy", side), lambda: c_copy(side, c).start())

    forward_xy, back_xy = mat[0:128, :], mat[128:256, :]
    forward_z, back_z = mat[256:512, :], mat[512:768, :]

    greeted = sum(side[name].astype(jnp.int32) for name in names for side in (below, above))
    greeted = greeted + (1 if detour else 0)
    waiting, cornering = list(relayed), list(order)
    for at, c in enumerate(order):
        in_copies[c].wait()
        for start in range(c * chunk, (c + 1) * chunk, STEP):
            lanes = slice(start, start + STEP)
            g00, g11, g22, g01, g02, g12 = [metric[k : k + 1, lanes] for k in range(6)]
            pairs = [split(u[comp, :, :, lanes].reshape(64, STEP)) for comp in range(comps)]
            planes = [
                product(forward_xy, jnp.concatenate([high, low, high, low], axis=0))
                for high, low in pairs
            ]
            grads_z = along_lanes(pairs, forward_z)
            sums, z_pairs = [], []
            for both, grad_z in zip(planes, grads_z):
                grad_x, grad_y = both[:64], both[64:]
                flux_x = g00 * grad_x + g01 * grad_y + g02 * grad_z
                flux_y = g01 * grad_x + g11 * grad_y + g12 * grad_z
                x_high, x_low = split(flux_x)
                y_high, y_low = split(flux_y)
                z_pairs.append(split(g02 * grad_x + g12 * grad_y + g22 * grad_z))
                sums.append(
                    product(back_xy, jnp.concatenate([x_high, y_high, x_low, y_low], axis=0))
                )
            backs_z = along_lanes(z_pairs, back_z)
            weight = jnp.concatenate([scale[0:64, :]] * (STEP // LANES), axis=1)
            for comp in range(comps):
                twice = sums[comp]
                terms = twice[:64] + twice[64:] + weight * backs_z[comp]
                terms = terms.reshape(8, 8, STEP)
                local[comp, :, :, lanes] = terms
                for n in range(8):
                    y_out[0, comp, n : n + 1, lanes] = terms[n, 7:8]
                    y_out[1, comp, n : n + 1, lanes] = terms[n, 0:1]
                    tile, row = seat(comp, n)
                    x_out[0, tile, row : row + 1, lanes] = terms[7, n : n + 1]
                    x_out[1, tile, row : row + 1, lanes] = terms[0, n : n + 1]
        if at == 0:
            pl.semaphore_wait(barrier, greeted)
        for side in range(2):
            when_do(target("gx", side), lambda: x_copy(side, c).start())
            when_do(target("gy", side), lambda: y_copy(side, c).start())
        if at > 1:
            send_bulk(order[at - 2])
        if at >= LAG and cornering:
            corners(cornering.pop(0))
        if at >= LAG + 1 and waiting:
            forward(waiting.pop(0))
    for c in order[-2:]:
        send_bulk(c)
    while waiting or cornering:
        if cornering:
            corners(cornering.pop(0))
        if waiting:
            forward(waiting.pop(0))

    def xy_sum(comp, n, lanes):
        value = local[comp, n, :, lanes]
        from_below = y_in[0, comp, n : n + 1, lanes]
        from_above = y_in[1, comp, n : n + 1, lanes]
        if n in (0, 7):
            x_side = 0 if n == 0 else 1
            at_row = 2 * comp + x_side
            seats = [seat(comp, m) for m in range(8)]
            rows = [x_in[x_side, tile, row : row + 1, lanes] for tile, row in seats]
            value = value + jnp.concatenate(rows, axis=0)
            from_below = from_below + corner_in[0, at_row : at_row + 1, lanes]
            from_above = from_above + corner_in[1, at_row : at_row + 1, lanes]
        where = lax.broadcasted_iota(jnp.int32, value.shape, 0)
        value = value + jnp.where(where == 0, from_below, 0.0)
        return value + jnp.where(where == 7, from_above, 0.0)

    def arrived(c):
        for side in range(2):
            when_do(source("gx", side), lambda: bulk_copy(side, c).wait_recv())
            when_do(source("gy", side), lambda: y_copy(side, c).wait_recv())
            when_do(source("gy", side), lambda: c_copy(side, c).wait_recv())

    def finish(first, last):
        for comp in range(comps):
            for n in range(8):
                value = xy_sum(comp, n, slice(max(first - LANES, 0), min(last + LANES, total)))
                if first == 0:
                    value = jnp.concatenate([z_in[0, comp, n], value], axis=1)
                if last == total:
                    value = jnp.concatenate([value, z_in[1, comp, n]], axis=1)
                width = value.shape[1]
                before = pltpu.roll(value, 1, 1)[:, LANES:-LANES]
                after = pltpu.roll(value, width - 1, 1)[:, LANES:-LANES]
                position = lax.broadcasted_iota(jnp.int32, before.shape, 1) % 8
                extra = jnp.where(position == 7, after, jnp.where(position == 0, before, 0.0))
                out[comp, n, :, first:last] = value[:, LANES:-LANES] + extra

    edge = order[:2] if count > 1 else order
    group = min(2 * chunk, total)
    groups = list(range(total // group))
    here = set()
    z_here = False
    for at, c in enumerate(order):
        arrived(c)
        here.add(c)
        if at == len(edge) - 1:
            for side in range(2):
                lanes = slice(total - LANES, total) if side == 0 else slice(0, LANES)
                for comp in range(comps):
                    for n in range(8):
                        z_out[side, comp, n] = xy_sum(comp, n, lanes)
                when_do(target("gz", side), lambda: z_copy(side).start())
        for g in list(groups):
            first, last = g * group // chunk, (g + 1) * group // chunk
            if all(i in here for i in range(max(first - 1, 0), min(last + 1, count))):
                groups.remove(g)
                ends = g * group, (g + 1) * group
                if not z_here and (ends[0] == 0 or ends[1] == total):
                    z_here = True
                    for side in range(2):
                        when_do(source("gz", side), lambda: z_copy(side).wait_recv())
                finish(*ends)

    for c in order:
        for side in range(2):
            when_do(target("gx", side), lambda: x_copy(side, c).wait_send())
            when_do(target("gx", side), lambda: bulk_copy(side, c).wait_send())
            when_do(target("gy", side), lambda: y_copy(side, c).wait_send())
            when_do(target("gy", side), lambda: c_copy(side, c).wait_send())
    for side in range(2):
        when_do(target("gz", side), lambda: z_copy(side).wait_send())
        for c in relayed:
            when_do(place["gx"] == by_way_of(side), lambda: onward_copy(side, c).wait_send())


def local_part(sizes, nodal_scalar_values, geometry):
    comps, _, _, total = nodal_scalar_values.shape
    chunk = min(256, total)
    count = total // chunk
    matrices, scales = tables()
    f32 = jnp.float32
    dma = pltpu.SemaphoreType.DMA
    any_space = pl.BlockSpec(memory_space=pl.ANY)
    return pl.pallas_call(
        functools.partial(kernel, sizes, chunk),
        out_shape=pltpu.VMEM(nodal_scalar_values.shape, f32),
        in_specs=[any_space] * 4,
        out_specs=pl.BlockSpec(memory_space=pltpu.VMEM),
        scratch_shapes=[
            pltpu.VMEM(nodal_scalar_values.shape, f32),
            pltpu.VMEM(geometry.shape, f32),
            pltpu.VMEM(matrices.shape, jnp.bfloat16),
            pltpu.VMEM(scales.shape, f32),
            pltpu.VMEM((8, total), f32),
            pltpu.VMEM(nodal_scalar_values.shape, f32),
            pltpu.VMEM((2, comps, 8, total), f32),
            pltpu.VMEM((2, comps, 8, total), f32),
            pltpu.VMEM((2, comps, 8, total), f32),
            pltpu.VMEM((2, comps, 8, total), f32),
            pltpu.VMEM((2, 8, total), f32),
            pltpu.VMEM((2, 8, total), f32),
            pltpu.VMEM((2, comps, 8, 8, LANES), f32),
            pltpu.VMEM((2, comps, 8, 8, LANES), f32),
            pltpu.VMEM((comps - 1, 8, total), f32),
            dma((count,)),
            dma((3,)),
            dma((2, count)),
            dma((2, count)),
            dma((2, count)),
            dma((2, count)),
            dma((2, count)),
            dma((2, count)),
            dma((2,)),
            dma((2,)),
            dma((count,)),
            dma((count,)),
            dma((2, count)),
            dma((2, count)),
        ],
        compiler_params=pltpu.CompilerParams(collective_id=0, has_side_effects=True),
        name="poisson",
    )(nodal_scalar_values, geometry, jnp.asarray(matrices), jnp.asarray(scales))


def solution(mesh):
    return jax.shard_map(
        functools.partial(local_part, dict(mesh.shape)),
        mesh=mesh,
        in_specs=(P(None, "gx", "gy", "gz"), P(None, "gx", "gy", "gz")),
        out_specs=P(None, "gx", "gy", "gz"),
        check_vma=False,
    )
```

```python
import functools

import jax
import jax.numpy as jnp
import numpy as np
from jax import lax
from jax.experimental import pallas as pl
from jax.experimental.pallas import tpu as pltpu
from jax.sharding import PartitionSpec as P

interior_points = [
    -0.8717401485096066,
    -0.5917001814331423,
    -0.2092992179024789,
    0.2092992179024789,
    0.5917001814331423,
    0.8717401485096066,
]
MESH = pl.DeviceIdType.MESH
STEP = 256
LANES = 128
X_FIRST = True
LAG = 5


def legendre_seven(point):
    previous = 1.0
    current = point
    for order in range(1, 7):
        following = ((2 * order + 1) * point * current - order * previous) / (order + 1)
        previous = current
        current = following
    return current


def gll_tables():
    degree = 7
    points = [-1.0] + interior_points + [1.0]
    values = [legendre_seven(point) for point in points]
    node_count = degree + 1
    weights = np.array([2.0 / (degree * (degree + 1) * value * value) for value in values])
    derivative = np.zeros((node_count, node_count))
    for row_index in range(node_count):
        for col_index in range(node_count):
            if row_index != col_index:
                derivative[row_index, col_index] = values[row_index] / (
                    values[col_index] * (points[row_index] - points[col_index])
                )
    derivative[0, 0] = -degree * (degree + 1) / 4.0
    derivative[node_count - 1, node_count - 1] = degree * (degree + 1) / 4.0
    return (derivative, weights)


def halves(table):
    table = np.asarray(table, np.float32)
    high = table.astype(jnp.bfloat16)
    low = (table - high.astype(np.float32)).astype(jnp.bfloat16)
    return high, low


def tables():
    derivative, weights = gll_tables()
    eye = np.eye(8)
    plane_weight = np.kron(weights, weights)
    forward_xy = np.concatenate([np.kron(derivative, eye), np.kron(eye, derivative)], axis=0)
    back_xy = np.concatenate([np.kron(derivative.T, eye), np.kron(eye, derivative.T)], axis=1)
    back_xy = back_xy * np.tile(plane_weight, 2)[None, :]
    forward_z = np.kron(np.eye(16), derivative.T)
    back_z = np.kron(np.eye(16), derivative)
    high, low = halves(forward_xy)
    forward_xy = np.concatenate([high, high, low, low], axis=1)
    high, low = halves(back_xy)
    back_xy = np.concatenate(
        [np.concatenate([high, high], axis=1), np.concatenate([low, low], axis=1)], axis=0
    )
    high, low = halves(forward_z)
    forward_z = np.tile(np.concatenate([high, low], axis=1), (2, 1))
    high, low = halves(back_z)
    back_z = np.tile(np.concatenate([high, low], axis=1), (2, 1))
    matrices = np.concatenate([forward_xy, back_xy, forward_z, back_z], axis=0)
    plane = np.repeat(plane_weight[:, None], LANES, axis=1)
    along = np.repeat(np.tile(weights, LANES // 8)[None, :], 8, axis=0)
    scales = np.concatenate([plane, along], axis=0).astype(np.float32)
    return matrices, scales


def seat(comp, m):
    if m in (0, 7):
        return 0, 2 * comp + (1 if m == 7 else 0)
    if comp:
        return comp, m - 1
    return (m - 1) // 2, 6 + (m - 1) % 2


def split(value):
    high = value.astype(jnp.bfloat16)
    low = (value - high.astype(jnp.float32)).astype(jnp.bfloat16)
    return high, low


def product(left, right):
    return jnp.dot(left, right, preferred_element_type=jnp.float32)


def along_lanes(pairs, table):
    rows, width = pairs[0][0].shape
    spans = [slice(start, start + LANES) for start in range(0, width, LANES)]
    stacked = [
        jnp.concatenate([high[:, span], low[:, span]], axis=1)
        for high, low in pairs
        for span in spans
    ]
    twice = product(jnp.concatenate(stacked, axis=0), table)
    once = twice[:, :LANES] + twice[:, LANES:]
    pieces = [once[at * rows : (at + 1) * rows] for at in range(len(stacked))]
    return [
        jnp.concatenate(pieces[at : at + len(spans)], axis=1)
        for at in range(0, len(pieces), len(spans))
    ]


def kernel(
    sizes,
    chunk,
    u_hbm,
    geo_hbm,
    mat_hbm,
    scale_hbm,
    out,
    u,
    geo,
    mat,
    scale,
    metric,
    local,
    x_out,
    y_out,
    x_in,
    y_in,
    corner_out,
    corner_in,
    z_out,
    z_in,
    relay,
    in_sem,
    const_sem,
    x_send,
    x_recv,
    y_send,
    y_recv,
    c_send,
    c_recv,
    z_send,
    z_recv,
    r_send,
    r_recv,
    b_send,
    b_recv,
):
    comps, _, _, total = u.shape
    count = total // chunk
    order = [0] + ([count - 1] if count > 1 else []) + list(range(1, count - 1))
    names = ("gx", "gy", "gz")
    place = {name: lax.axis_index(name) for name in names}
    below = {name: place[name] > 0 for name in names}
    above = {name: place[name] < sizes[name] - 1 for name in names}

    const_copies = [
        pltpu.make_async_copy(mat_hbm, mat, const_sem.at[0]),
        pltpu.make_async_copy(scale_hbm, scale, const_sem.at[1]),
        pltpu.make_async_copy(geo_hbm, geo, const_sem.at[2]),
    ]
    for copy in const_copies:
        copy.start()
    in_copies = {}
    for c in order:
        span = pl.ds(c * chunk, chunk)
        in_copies[c] = pltpu.make_async_copy(
            u_hbm.at[:, :, :, span], u.at[:, :, :, span], in_sem.at[c]
        )
        in_copies[c].start()

    barrier = pltpu.get_barrier_semaphore()
    for name in names:
        for there, by in ((below[name], -1), (above[name], 1)):

            @pl.when(there)
            def _(name=name, by=by):
                pl.semaphore_signal(
                    barrier, inc=1, device_id={name: place[name] + by}, device_id_type=MESH
                )

    detour = sizes["gx"] == 4
    relayed = order[: count * 3 // 4] if detour else []
    opposite = lax.rem(place["gx"] + 2, 4)
    if detour:
        pl.semaphore_signal(barrier, inc=1, device_id={"gx": opposite}, device_id_type=MESH)

    for side in range(2):
        there = below if side == 0 else above

        @pl.when(jnp.logical_not(there["gx"]))
        def _(side=side):
            x_in[side] = jnp.zeros(x_in.shape[1:], jnp.float32)

        @pl.when(jnp.logical_not(there["gy"]))
        def _(side=side):
            y_in[side] = jnp.zeros(y_in.shape[1:], jnp.float32)
            corner_in[side] = jnp.zeros(corner_in.shape[1:], jnp.float32)

        @pl.when(jnp.logical_not(there["gz"]))
        def _(side=side):
            z_in[side] = jnp.zeros(z_in.shape[1:], jnp.float32)

    for copy in const_copies:
        copy.wait()

    rows = jnp.concatenate(
        [geo[k, 0] for k in range(6)] + [jnp.zeros((2, geo.shape[-1]), jnp.float32)], axis=0
    )
    lane = lax.broadcasted_iota(jnp.int32, (8, LANES), 1)
    for tile in range(total // LANES):
        first = tile * (LANES // 8)
        block = rows[:, first // LANES * LANES : first // LANES * LANES + LANES]
        spread = jnp.take_along_axis(block, lane // 8 + first % LANES, axis=1)
        metric[:, tile * LANES : (tile + 1) * LANES] = spread * scale[64:72, :]

    def x_copy(side, c):
        span = pl.ds(c * chunk, chunk)
        return pltpu.make_async_remote_copy(
            x_out.at[side, 0, :, span],
            x_in.at[side, 0, :, span],
            x_send.at[side, c],
            x_recv.at[side, c],
            device_id={"gx": place["gx"] + (1 if side == 0 else -1)},
            device_id_type=MESH,
        )

    def bulk_copy(side, c):
        span = pl.ds(c * chunk, chunk)
        return pltpu.make_async_remote_copy(
            x_out.at[side, 1:, :, span],
            x_in.at[side, 1:, :, span],
            b_send.at[side, c],
            b_recv.at[side, c],
            device_id={"gx": place["gx"] + (1 if side == 0 else -1)},
            device_id_type=MESH,
        )

    def middle(side):
        return place["gx"] == 1 + side

    def by_way_of(side):
        return 3 * (1 - side) if X_FIRST else 3 * side

    def hop_copy(side, c):
        span = pl.ds(c * chunk, chunk)
        return pltpu.make_async_remote_copy(
            x_out.at[side, 1:, :, span],
            relay.at[:, :, span],
            b_send.at[side, c],
            r_recv.at[c],
            device_id={"gx": by_way_of(side)},
            device_id_type=MESH,
        )

    def onward_copy(side, c):
        span = pl.ds(c * chunk, chunk)
        return pltpu.make_async_remote_copy(
            relay.at[:, :, span],
            x_in.at[side, 1:, :, span],
            r_send.at[c],
            b_recv.at[side, c],
            device_id={"gx": 2 - side},
            device_id_type=MESH,
        )

    def forward(c):
        for side in range(2):

            @pl.when(place["gx"] == by_way_of(side))
            def _(side=side):
                hop_copy(side, c).wait_recv()
                onward_copy(side, c).start()

    def send_bulk(c):
        for side in range(2):
            if c in relayed:
                straight = jnp.logical_and(target("gx", side), jnp.logical_not(middle(side)))
                when_do(straight, lambda: bulk_copy(side, c).start())
                when_do(middle(side), lambda: hop_copy(side, c).start())
            else:
                when_do(target("gx", side), lambda: bulk_copy(side, c).start())

    def y_copy(side, c):
        span = pl.ds(c * chunk, chunk)
        return pltpu.make_async_remote_copy(
            y_out.at[side, :, :, span],
            y_in.at[side, :, :, span],
            y_send.at[side, c],
            y_recv.at[side, c],
            device_id={"gy": place["gy"] + (1 if side == 0 else -1)},
            device_id_type=MESH,
        )

    def c_copy(side, c):
        span = pl.ds(c * chunk, chunk)
        return pltpu.make_async_remote_copy(
            corner_out.at[side, :, span],
            corner_in.at[side, :, span],
            c_send.at[side, c],
            c_recv.at[side, c],
            device_id={"gy": place["gy"] + (1 if side == 0 else -1)},
            device_id_type=MESH,
        )

    def z_copy(side):
        return pltpu.make_async_remote_copy(
            z_out.at[side],
            z_in.at[side],
            z_send.at[side],
            z_recv.at[side],
            device_id={"gz": place["gz"] + (1 if side == 0 else -1)},
            device_id_type=MESH,
        )

    def target(name, side):
        return above[name] if side == 0 else below[name]

    def source(name, side):
        return below[name] if side == 0 else above[name]

    def when_do(condition, act):
        @pl.when(condition)
        def _():
            act()

    def corners(c):
        lanes = slice(c * chunk, (c + 1) * chunk)
        for side in range(2):
            when_do(source("gx", side), lambda: x_copy(side, c).wait_recv())
        for side in range(2):
            for comp in range(comps):
                for x_side in range(2):
                    at_row = 2 * comp + x_side
                    tile, row = seat(comp, 7 if side == 0 else 0)
                    corner_out[side, at_row : at_row + 1, lanes] = x_in[
                        x_side, tile, row : row + 1, lanes
                    ]
            when_do(target("gy", side), lambda: c_copy(side, c).start())

    forward_xy, back_xy = mat[0:128, :], mat[128:256, :]
    forward_z, back_z = mat[256:512, :], mat[512:768, :]

    greeted = sum(side[name].astype(jnp.int32) for name in names for side in (below, above))
    greeted = greeted + (1 if detour else 0)
    waiting, cornering = list(relayed), list(order)
    for at, c in enumerate(order):
        in_copies[c].wait()
        for start in range(c * chunk, (c + 1) * chunk, STEP):
            lanes = slice(start, start + STEP)
            g00, g11, g22, g01, g02, g12 = [metric[k : k + 1, lanes] for k in range(6)]
            pairs = [split(u[comp, :, :, lanes].reshape(64, STEP)) for comp in range(comps)]
            planes = [
                product(forward_xy, jnp.concatenate([high, low, high, low], axis=0))
                for high, low in pairs
            ]
            grads_z = along_lanes(pairs, forward_z)
            sums, z_pairs = [], []
            for both, grad_z in zip(planes, grads_z):
                grad_x, grad_y = both[:64], both[64:]
                flux_x = g00 * grad_x + g01 * grad_y + g02 * grad_z
                flux_y = g01 * grad_x + g11 * grad_y + g12 * grad_z
                x_high, x_low = split(flux_x)
                y_high, y_low = split(flux_y)
                z_pairs.append(split(g02 * grad_x + g12 * grad_y + g22 * grad_z))
                sums.append(
                    product(back_xy, jnp.concatenate([x_high, y_high, x_low, y_low], axis=0))
                )
            backs_z = along_lanes(z_pairs, back_z)
            weight = jnp.concatenate([scale[0:64, :]] * (STEP // LANES), axis=1)
            for comp in range(comps):
                twice = sums[comp]
                terms = twice[:64] + twice[64:] + weight * backs_z[comp]
                terms = terms.reshape(8, 8, STEP)
                local[comp, :, :, lanes] = terms
                for n in range(8):
                    y_out[0, comp, n : n + 1, lanes] = terms[n, 7:8]
                    y_out[1, comp, n : n + 1, lanes] = terms[n, 0:1]
                    tile, row = seat(comp, n)
                    x_out[0, tile, row : row + 1, lanes] = terms[7, n : n + 1]
                    x_out[1, tile, row : row + 1, lanes] = terms[0, n : n + 1]
        if at == 0:
            pl.semaphore_wait(barrier, greeted)
        for side in range(2):
            when_do(target("gx", side), lambda: x_copy(side, c).start())
            when_do(target("gy", side), lambda: y_copy(side, c).start())
        if at > 2:
            send_bulk(order[at - 3])
        if at >= LAG and cornering:
            corners(cornering.pop(0))
        if at >= LAG + 1 and waiting:
            forward(waiting.pop(0))
    for c in order[-3:]:
        send_bulk(c)
    while waiting or cornering:
        if cornering:
            corners(cornering.pop(0))
        if waiting:
            forward(waiting.pop(0))

    def xy_sum(comp, n, lanes):
        value = local[comp, n, :, lanes]
        from_below = y_in[0, comp, n : n + 1, lanes]
        from_above = y_in[1, comp, n : n + 1, lanes]
        if n in (0, 7):
            x_side = 0 if n == 0 else 1
            at_row = 2 * comp + x_side
            seats = [seat(comp, m) for m in range(8)]
            rows = [x_in[x_side, tile, row : row + 1, lanes] for tile, row in seats]
            value = value + jnp.concatenate(rows, axis=0)
            from_below = from_below + corner_in[0, at_row : at_row + 1, lanes]
            from_above = from_above + corner_in[1, at_row : at_row + 1, lanes]
        where = lax.broadcasted_iota(jnp.int32, value.shape, 0)
        value = value + jnp.where(where == 0, from_below, 0.0)
        return value + jnp.where(where == 7, from_above, 0.0)

    def arrived(c):
        for side in range(2):
            when_do(source("gx", side), lambda: bulk_copy(side, c).wait_recv())
            when_do(source("gy", side), lambda: y_copy(side, c).wait_recv())
            when_do(source("gy", side), lambda: c_copy(side, c).wait_recv())

    def finish(first, last):
        for comp in range(comps):
            for n in range(8):
                value = xy_sum(comp, n, slice(max(first - LANES, 0), min(last + LANES, total)))
                if first == 0:
                    value = jnp.concatenate([z_in[0, comp, n], value], axis=1)
                if last == total:
                    value = jnp.concatenate([value, z_in[1, comp, n]], axis=1)
                width = value.shape[1]
                before = pltpu.roll(value, 1, 1)[:, LANES:-LANES]
                after = pltpu.roll(value, width - 1, 1)[:, LANES:-LANES]
                position = lax.broadcasted_iota(jnp.int32, before.shape, 1) % 8
                extra = jnp.where(position == 7, after, jnp.where(position == 0, before, 0.0))
                out[comp, n, :, first:last] = value[:, LANES:-LANES] + extra

    edge = order[:2] if count > 1 else order
    group = min(2 * chunk, total)
    groups = list(range(total // group))
    here = set()
    z_here = False
    for at, c in enumerate(order):
        arrived(c)
        here.add(c)
        if at == len(edge) - 1:
            for side in range(2):
                lanes = slice(total - LANES, total) if side == 0 else slice(0, LANES)
                for comp in range(comps):
                    for n in range(8):
                        z_out[side, comp, n] = xy_sum(comp, n, lanes)
                when_do(target("gz", side), lambda: z_copy(side).start())
        for g in list(groups):
            first, last = g * group // chunk, (g + 1) * group // chunk
            if all(i in here for i in range(max(first - 1, 0), min(last + 1, count))):
                groups.remove(g)
                ends = g * group, (g + 1) * group
                if not z_here and (ends[0] == 0 or ends[1] == total):
                    z_here = True
                    for side in range(2):
                        when_do(source("gz", side), lambda: z_copy(side).wait_recv())
                finish(*ends)

    for c in order:
        for side in range(2):
            when_do(target("gx", side), lambda: x_copy(side, c).wait_send())
            when_do(target("gx", side), lambda: bulk_copy(side, c).wait_send())
            when_do(target("gy", side), lambda: y_copy(side, c).wait_send())
            when_do(target("gy", side), lambda: c_copy(side, c).wait_send())
    for side in range(2):
        when_do(target("gz", side), lambda: z_copy(side).wait_send())
        for c in relayed:
            when_do(place["gx"] == by_way_of(side), lambda: onward_copy(side, c).wait_send())


def local_part(sizes, nodal_scalar_values, geometry):
    comps, _, _, total = nodal_scalar_values.shape
    chunk = min(256, total)
    count = total // chunk
    matrices, scales = tables()
    f32 = jnp.float32
    dma = pltpu.SemaphoreType.DMA
    any_space = pl.BlockSpec(memory_space=pl.ANY)
    return pl.pallas_call(
        functools.partial(kernel, sizes, chunk),
        out_shape=pltpu.VMEM(nodal_scalar_values.shape, f32),
        in_specs=[any_space] * 4,
        out_specs=pl.BlockSpec(memory_space=pltpu.VMEM),
        scratch_shapes=[
            pltpu.VMEM(nodal_scalar_values.shape, f32),
            pltpu.VMEM(geometry.shape, f32),
            pltpu.VMEM(matrices.shape, jnp.bfloat16),
            pltpu.VMEM(scales.shape, f32),
            pltpu.VMEM((8, total), f32),
            pltpu.VMEM(nodal_scalar_values.shape, f32),
            pltpu.VMEM((2, comps, 8, total), f32),
            pltpu.VMEM((2, comps, 8, total), f32),
            pltpu.VMEM((2, comps, 8, total), f32),
            pltpu.VMEM((2, comps, 8, total), f32),
            pltpu.VMEM((2, 8, total), f32),
            pltpu.VMEM((2, 8, total), f32),
            pltpu.VMEM((2, comps, 8, 8, LANES), f32),
            pltpu.VMEM((2, comps, 8, 8, LANES), f32),
            pltpu.VMEM((comps - 1, 8, total), f32),
            dma((count,)),
            dma((3,)),
            dma((2, count)),
            dma((2, count)),
            dma((2, count)),
            dma((2, count)),
            dma((2, count)),
            dma((2, count)),
            dma((2,)),
            dma((2,)),
            dma((count,)),
            dma((count,)),
            dma((2, count)),
            dma((2, count)),
        ],
        compiler_params=pltpu.CompilerParams(collective_id=0, has_side_effects=True),
        name="poisson",
    )(nodal_scalar_values, geometry, jnp.asarray(matrices), jnp.asarray(scales))


def solution(mesh):
    return jax.shard_map(
        functools.partial(local_part, dict(mesh.shape)),
        mesh=mesh,
        in_specs=(P(None, "gx", "gy", "gz"), P(None, "gx", "gy", "gz")),
        out_specs=P(None, "gx", "gy", "gz"),
        check_vma=False,
    )
```
